32 devices in a mesh: dp: 8 (over z, y), sub: 4 (over x, core).
Axes of the slice: x: 2, y: 2, z: 4, core: 2. Of those that a mesh axis runs over, the one named last changes fastest.
Arguments:
- embeddings: bfloat16 [16384, 1024], P(('dp', 'sub')), may hold values from -6 to 6
- rotation: bfloat16 [1024, 1024], replicated, may hold values from -0.1875 to 0.1875
- centroids: bfloat16 [8, 1024], replicated, may hold values from -6 to 6
- assignments: int32 [16384], P(('dp', 'sub')), may hold values from 0 to 7
- codes: int32 [16384, 64], P(('dp', 'sub')), may hold values from 0 to 255
Outputs:
- gram: float32 [1024, 1024], P('sub')
- coarse_sums: float32 [8, 1024], P('dp', 'sub')
- codebook_sums: float32 [256, 1024], P(None, 'sub')
The draws below stay inside these ranges and needn't reach their ends.
All inputs are finite; a program needn't handle non-finite values.
Results may differ from the reference program's by a relative error of at most 0.0045.
Values may be sent and summed in bfloat16 or wider, within the bound.
A program may use at most 64 MiB of HBM per device.

```python
import math
import jax
import jax.numpy as jnp
import numpy as np
from jax import lax

D = 1024
M = 64
K = 256
VEC_DEV = 512
VECS = 16384
CENTS = 8
N_SUB = 4


def touch_ends(array, stream_key, smallest, top_value):
    longest = array.shape.index(max(array.shape))
    spots = []
    for shift in (0, 1):
        where = [jax.random.randint(jax.random.fold_in(stream_key, axis), (), 0, length) for axis, length in enumerate(array.shape)]
        where[longest] = (where[longest] + shift) % array.shape[longest]
        spots.append(tuple(where))
    return array.at[spots[0]].set(smallest).at[spots[1]].set(top_value)


def with_spikes(values, rng, source, target, blocks, factor):
    owner, partner = [(jnp.arange(values.shape[position]) // (values.shape[position] // blocks)).reshape([-1 if axis == position else 1 for axis in range(values.ndim)]) for position in (source, target)]
    chosen = jax.random.permutation(rng, blocks)[partner]
    strong = (owner == chosen) | (owner == (partner + blocks // 2) % blocks)
    return jnp.where(strong, factor * values, values)


def shard_levels(own_key, dims, cuts, least, high):
    def one(dim, blocks):
        heights = jax.random.uniform(jax.random.fold_in(jax.random.fold_in(own_key, 6), dim), (blocks,), jnp.float32, least / len(cuts), high / len(cuts))
        return jnp.repeat(jnp.exp(heights), dims[dim] // blocks).reshape((-1,) + (1,) * (len(dims) - dim - 1))

    loudness = one(*cuts[0])
    for cut in cuts[1:]:
        loudness = loudness * one(*cut)
    return loudness


def rank_table(count, lean):
    portions = [(1 << 20) // math.isqrt(grade ** lean) + 1 for grade in range(1, count + 1)]
    deviation = 1 + sum(portions) // (1 << 30)
    return np.cumsum(np.array([max(1, weight // deviation) for weight in portions]))


def ranked(key, extent, amount, lean):
    listing = rank_table(amount, lean)
    ticket = jax.random.randint(jax.random.fold_in(key, 1), extent, 0, int(listing[amount - 1]))
    grade = jnp.searchsorted(jnp.asarray(listing, jnp.int32), ticket, side="right")
    return jax.random.permutation(jax.random.fold_in(key, 2), amount)[grade].astype(jnp.int32)


def noise(own_key, dims, width, limit, cuts=(), kind=jnp.bfloat16):
    drawn = width * jax.random.normal(own_key, dims, jnp.float32)
    if cuts:
        drawn = drawn * shard_levels(own_key, dims, cuts, -0.22, 0.18)
    return jnp.clip(drawn, -limit, limit).astype(kind)


def heavy_noise(own_key, shape, deviation, most, split, heavy, kind=jnp.bfloat16):
    array = deviation * jax.random.normal(own_key, shape, jnp.float32)
    if split:
        array = array * shard_levels(own_key, shape, split, -0.22, 0.18)
    return jnp.clip(with_spikes(array, jax.random.fold_in(own_key, 3), *heavy), -most, most).astype(kind)


def setup_inputs(seed: int = 0) -> dict:
    arg_keys = jax.random.split(jax.random.key(seed), 6)
    return {
        "embeddings": heavy_noise(arg_keys[0], (VECS, D), 1.0, 6.0, ((0, 32),), (0, 1, 32, 2.75)),
        "rotation": noise(arg_keys[1], (D, D), D ** -0.5, 0.1875),
        "centroids": noise(arg_keys[2], (CENTS, D), 1.0, 6.0),
        "assignments": touch_ends(ranked(arg_keys[3], (VECS,), CENTS, 1), jax.random.fold_in(arg_keys[3], 3), 0, CENTS - 1).astype(jnp.int32),
        "codes": touch_ends(jax.random.randint(arg_keys[4], (VECS, M), 0, K), jax.random.fold_in(arg_keys[4], 1), 0, K - 1).astype(jnp.int32),
    }


def reference(embeddings, rotation, centroids, assignments, codes):
    block = VEC_DEV * N_SUB
    count = VECS // block
    subw = D // M
    emb_blocks = embeddings.reshape(count, block, D)
    asg_blocks = assignments.reshape(count, block)
    code_blocks = codes.reshape(count, block, M)
    offsets = (jnp.arange(M, dtype=jnp.int32) * K)[None, :]

    def advance(carry, item):
        gram, coarse, book = carry
        rows, asg, code = item
        groups = rows.reshape(N_SUB, VEC_DEV, D).astype(jnp.float32)
        parts = jnp.einsum("gvi,gvj->gij", groups, groups).astype(jnp.bfloat16)
        gram = gram + jnp.sum(parts.astype(jnp.float32), axis=0)
        rotated = jnp.dot(rows, rotation, preferred_element_type=jnp.float32)
        residual = (rotated - centroids[asg].astype(jnp.float32)).astype(jnp.bfloat16)
        wide = residual.astype(jnp.float32)
        coarse = coarse + jax.ops.segment_sum(wide, asg, num_segments=CENTS)
        pieces = wide.reshape(block * M, subw)
        labels = (code + offsets).reshape(block * M).astype(jnp.int32)
        book = book + jax.ops.segment_sum(pieces, labels, num_segments=M * K)
        return (gram, coarse, book), None

    start = (jnp.zeros((D, D), jnp.float32), jnp.zeros((CENTS, D), jnp.float32),
             jnp.zeros((M * K, subw), jnp.float32))
    (gram, coarse, book), _ = lax.scan(advance, start, (emb_blocks, asg_blocks, code_blocks))
    gram = gram / VECS
    coarse = coarse * (CENTS / VECS) ** 0.5
    book = book.reshape(M, K, subw).transpose(1, 0, 2).reshape(K, D) * (K / VECS) ** 0.5
    return gram, coarse, book
```

```python
import functools

import jax
import jax.numpy as jnp
from jax import lax
from jax.experimental import pallas as pl
from jax.experimental.pallas import tpu as pltpu
from jax.sharding import PartitionSpec as P

M = 64
K = 256
LANES = 128
PIECES = 2


def contract_rows(left, right):
    return lax.dot_general(
        left, right, (((0,), (0,)), ((), ())), preferred_element_type=jnp.float32
    )


def plain_per_device(embeddings, rotation, centroids, assignments, codes):
    vec_rows, width = embeddings.shape
    cent_total = centroids.shape[0]
    sub_count = lax.axis_size("sub")
    dp_count = lax.axis_size("dp")
    total_rows = vec_rows * sub_count * dp_count
    gram_part = lax.psum_scatter(
        contract_rows(embeddings, embeddings).astype(jnp.bfloat16),
        "sub",
        scatter_dimension=0,
        tiled=True,
    ).astype(jnp.float32)
    rotated = jnp.dot(embeddings, rotation, preferred_element_type=jnp.float32)
    labels = lax.broadcasted_iota(jnp.int32, (1, cent_total), 1)
    select = (assignments[:, None] == labels).astype(jnp.bfloat16)
    base = jnp.dot(select, centroids, preferred_element_type=jnp.float32)
    residual = (rotated - base).astype(jnp.bfloat16)
    everything = contract_rows(select, residual)
    columns = lax.psum_scatter(
        everything.astype(jnp.bfloat16), "sub", scatter_dimension=1, tiled=True
    ).astype(jnp.float32)
    coarse = lax.psum_scatter(columns, "dp", scatter_dimension=0, tiled=True)
    coarse_sums = coarse * (cent_total / total_rows) ** 0.5
    code_words = codes.astype(jnp.bfloat16)
    moved, moved_codes = (
        lax.all_to_all(residual, "sub", split_axis=1, concat_axis=0, tiled=True),
        lax.all_to_all(code_words, "sub", split_axis=1, concat_axis=0, tiled=True),
    )
    local_m = codes.shape[1] // sub_count
    subw = width // codes.shape[1]
    owner_codes = moved_codes.astype(jnp.int32)
    gathered_rows = moved.shape[0]
    words = lax.broadcasted_iota(jnp.int32, (1, 1, K), 2)
    onehot = (owner_codes[:, :, None] == words).astype(jnp.bfloat16)
    pieces = moved.reshape(gathered_rows, local_m, subw)
    book_blocks = jnp.einsum("rmk,rms->kms", onehot, pieces, preferred_element_type=jnp.float32)
    book_local = book_blocks.reshape(K, local_m * subw)
    gram_sum, book_sum = lax.psum((gram_part, book_local), "dp")
    gram = gram_sum / total_rows
    codebook_sums = book_sum * (K / total_rows) ** 0.5
    return (gram, coarse_sums, codebook_sums)


def kernel(
    ns, nd, total_rows,
    emb, rot, cent, asg, codes,
    gram_o, coarse_o, book_o,
    gs1, gr1, gs2, gr2, gacc, gs3, gr3, gag,
    res, codes_t, ball, br1, bs2, br2, bacc, bs3, br3, bag, cs3, cr3,
    ssem, rsem,
):
    rows, width = emb.shape
    cents = cent.shape[0]
    nh = ns // 2
    gr = width // ns
    pr = gr // PIECES
    cr = pr // nd
    bc = width // ns
    kr = K // nd
    f32, bf16 = jnp.float32, jnp.bfloat16
    d = lax.axis_index("dp")
    s = lax.axis_index("sub")
    half, par = s // 2, lax.rem(s, 2)
    other = 1 - par
    pair = (d, half * 2 + other)

    def mate(k):
        return lax.rem(half + k, nh)

    def peer(k):
        return lax.rem(d + k, nd)

    barrier = pltpu.get_barrier_semaphore()
    greet = [pair]
    greet += [(d, mate(k) * 2 + par) for k in range(1, nh)]
    greet += [(peer(k), s) for k in range(1, nd)]
    for who in greet:
        pl.semaphore_signal(barrier, inc=1, device_id=who, device_id_type=pl.DeviceIdType.MESH)

    started = []

    def send(src, dst, who):
        n = len(started)
        copy = pltpu.make_async_remote_copy(
            src_ref=src, dst_ref=dst, send_sem=ssem.at[n], recv_sem=rsem.at[n],
            device_id=who, device_id_type=pl.DeviceIdType.MESH,
        )
        copy.start()
        started.append(copy)
        return copy

    def gram_block(q):
        cols = pl.ds(pl.multiple_of(q * gr, gr), gr)
        return contract_rows(emb[:, cols], emb[...]).astype(bf16)

    first = []
    for k in range(nh):
        i = mate(nh - 1 - k)
        gs1[k] = gram_block(i * 2 + other)
        if k == 0:
            pl.semaphore_wait(barrier, len(greet))
        first.append(send(gs1.at[k], gr1.at[k], pair))
    g2 = {}
    for k in range(nh):
        i = mate(nh - 1 - k)
        own = gram_block(i * 2 + par)
        first[k].wait_recv()
        both = own.astype(f32) + gr1[k].astype(f32)
        if k < nh - 1:
            gs2[k] = both.astype(bf16)
            who = (d, i * 2 + par)
            for h in range(PIECES):
                span = pl.ds(h * pr, pr)
                g2[k, h] = send(gs2.at[k, span], gr2.at[k, span], who)
        else:
            gacc[...] = both

    asg_row = asg[...]
    select = (asg_row == lax.broadcasted_iota(jnp.int32, (cents, rows), 0)).astype(f32).astype(bf16)
    for c in range(width // 256):
        cols = slice(c * 256, (c + 1) * 256)
        rotated = jnp.dot(emb[...], rot[:, cols], preferred_element_type=f32)
        base = contract_rows(select, cent[:, cols])
        res[:, cols] = (rotated - base).astype(bf16)
    m = codes.shape[1]
    eye = (
        lax.broadcasted_iota(jnp.int32, (m, m), 0) == lax.broadcasted_iota(jnp.int32, (m, m), 1)
    ).astype(f32).astype(bf16)
    codes_t[...] = lax.dot_general(
        eye, codes[...].astype(f32).astype(bf16), (((1,), (1,)), ((), ())),
        preferred_element_type=f32,
    ).astype(jnp.int32)

    subw = width // m
    per = LANES // subw
    lane_owner = lax.broadcasted_iota(jnp.int32, (K, LANES), 1) // subw
    words = lax.broadcasted_iota(jnp.int32, (K, rows), 0)
    groups = bc // LANES

    def group_step(g, carry):
        q, off = g // groups, lax.rem(g, groups)
        part = res[:, pl.ds(pl.multiple_of(g * LANES, LANES), LANES)]
        names = codes_t[pl.ds(pl.multiple_of(g * per, per), per), :]
        total = jnp.zeros((K, LANES), f32)
        for j in range(per):
            hot = jnp.where(names[j : j + 1, :] == words, 1.0, 0.0).astype(bf16)
            got = jnp.dot(hot, part, preferred_element_type=f32)
            total = jnp.where(lane_owner == j, got, total)
        lanes = pl.ds(pl.multiple_of(off * LANES, LANES), LANES)
        ball[q, 0:K, lanes] = total
        return carry

    lax.fori_loop(0, width // LANES, group_step, 0)
    cpad = ball.shape[1] - K
    select_pad = (asg_row == lax.broadcasted_iota(jnp.int32, (cpad, rows), 0)).astype(f32).astype(bf16)
    for q in range(ns):
        ball[q, K : K + cpad, :] = jnp.dot(
            select_pad, res[:, q * bc : (q + 1) * bc], preferred_element_type=f32
        )

    b1 = []
    for k in range(nh):
        i = mate(nh - 1 - k)
        b1.append(send(ball.at[i * 2 + other], br1.at[k], pair))
    b2 = {}
    for k in range(nh):
        i = mate(nh - 1 - k)
        b1[k].wait_recv()
        both = ball[i * 2 + par] + br1[k]
        if k < nh - 1:
            bs2[k] = both.astype(bf16)
            b2[k] = send(bs2.at[k], br2.at[k], (d, i * 2 + par))
        else:
            bacc[...] = both

    g3 = {}
    for h in range(PIECES):
        span = pl.ds(h * pr, pr)
        total = gacc[span, :]
        for k in range(nh - 1):
            g2[k, h].wait_recv()
            total = total + gr2[k, span, :].astype(f32)
        gacc[span, :] = total
        gs3[h] = total.astype(bf16).reshape(nd, cr, width)
        for k in range(1, nd):
            g3[h, k] = send(gs3.at[h, peer(k)], gr3.at[h, k - 1], (peer(k), s))
    total = bacc[...]
    for k in range(nh - 1):
        b2[k].wait_recv()
        total = total + br2[k].astype(f32)
    bs3[...] = total[0:K].reshape(nd, kr, bc)
    cper = cents // nd
    for e in range(nd):
        cs3[e] = total[K + e * cper : K + (e + 1) * cper]
    b3, c3 = {}, {}
    for k in range(1, nd):
        b3[k] = send(bs3.at[peer(k)], br3.at[k - 1], (peer(k), s))
        c3[k] = send(cs3.at[peer(k)], cr3.at[k - 1], (peer(k), s))

    g4 = {}
    for h in range(PIECES):
        total = gacc[pl.ds(pl.multiple_of(h * pr + d * cr, cr), cr), :]
        for k in range(1, nd):
            g3[h, k].wait_recv()
            total = total + gr3[h, k - 1].astype(f32)
        gag[h, d] = total.astype(bf16)
        for k in range(1, nd):
            g4[h, k] = send(gag.at[h, d], gag.at[h, d], (peer(k), s))
    total = bs3[d]
    ctotal = cs3[d]
    for k in range(1, nd):
        b3[k].wait_recv()
        c3[k].wait_recv()
        total = total + br3[k - 1]
        ctotal = ctotal + cr3[k - 1]
    bag[d] = total.astype(bf16)
    b4 = {}
    for k in range(1, nd):
        b4[k] = send(bag.at[d], bag.at[d], (peer(k), s))
    coarse_o[...] = ctotal * (cents / total_rows) ** 0.5
    for h in range(PIECES):
        for k in range(1, nd):
            g4[h, k].wait_recv()
        gram_o[h * pr : (h + 1) * pr, :] = gag[h].astype(f32).reshape(pr, width) * (1.0 / total_rows)
    for k in range(1, nd):
        b4[k].wait_recv()
    book_o[...] = bag[...].astype(f32).reshape(K, bc) * (K / total_rows) ** 0.5
    for copy in started:
        copy.wait_send()


def fused_per_device(ns, nd, embeddings, rotation, centroids, assignments, codes):
    rows, width = embeddings.shape
    cents = centroids.shape[0]
    total_rows = rows * ns * nd
    nh = ns // 2
    gr = width // ns
    pr = gr // PIECES
    cr = pr // nd
    bc = width // ns
    cpad = -(-cents // 16) * 16
    f32, bf16 = jnp.float32, jnp.bfloat16
    far = max(nh - 1, 1)
    copies = nh + (nh - 1) * PIECES + nh + (nh - 1) + (nd - 1) * (2 * PIECES + 3)
    scratch = [
        pltpu.VMEM((nh, gr, width), bf16),
        pltpu.VMEM((nh, gr, width), bf16),
        pltpu.VMEM((far, gr, width), bf16),
        pltpu.VMEM((far, gr, width), bf16),
        pltpu.VMEM((gr, width), f32),
        pltpu.VMEM((PIECES, nd, cr, width), bf16),
        pltpu.VMEM((PIECES, nd - 1, cr, width), bf16),
        pltpu.VMEM((PIECES, nd, cr, width), bf16),
        pltpu.VMEM((rows, width), bf16),
        pltpu.VMEM((codes.shape[1], rows), jnp.int32),
        pltpu.VMEM((ns, K + cpad, bc), f32),
        pltpu.VMEM((nh, K + cpad, bc), f32),
        pltpu.VMEM((far, K + cpad, bc), bf16),
        pltpu.VMEM((far, K + cpad, bc), bf16),
        pltpu.VMEM((K + cpad, bc), f32),
        pltpu.VMEM((nd, K // nd, bc), f32),
        pltpu.VMEM((nd - 1, K // nd, bc), f32),
        pltpu.VMEM((nd, K // nd, bc), bf16),
        pltpu.VMEM((nd, cents // nd, bc), f32),
        pltpu.VMEM((nd - 1, cents // nd, bc), f32),
        pltpu.SemaphoreType.DMA((copies,)),
        pltpu.SemaphoreType.DMA((copies,)),
    ]
    vmem = pl.BlockSpec(memory_space=pltpu.VMEM)
    return tuple(
        pl.pallas_call(
            functools.partial(kernel, ns, nd, total_rows),
            out_shape=(
                jax.ShapeDtypeStruct((gr, width), f32),
                jax.ShapeDtypeStruct((cents // nd, bc), f32),
                jax.ShapeDtypeStruct((K, bc), f32),
            ),
            in_specs=[vmem] * 5,
            out_specs=(vmem,) * 3,
            scratch_shapes=scratch,
            compiler_params=pltpu.CompilerParams(
                collective_id=0, has_side_effects=True, vmem_limit_bytes=56 * 1024 * 1024
            ),
        )(embeddings, rotation, centroids, assignments.reshape(1, rows), codes)
    )


def solution(mesh):
    ns, nd = mesh.shape["sub"], mesh.shape["dp"]

    def per_device(embeddings, rotation, centroids, assignments, codes):
        rows, width = embeddings.shape
        cents = centroids.shape[0]
        fits = (
            ns % 2 == 0
            and nd > 1
            and width % (ns * PIECES * nd * 16) == 0
            and width % (ns * 2 * LANES // 2) == 0
            and K % (nd * 16) == 0
            and cents % nd == 0
            and cents % 8 == 0
            and LANES % (width // M) == 0
        )
        if fits:
            return fused_per_device(ns, nd, embeddings, rotation, centroids, assignments, codes)
        return plain_per_device(embeddings, rotation, centroids, assignments, codes)

    return jax.shard_map(
        per_device,
        mesh=mesh,
        in_specs=(P(("dp", "sub"), None), P(), P(), P(("dp", "sub")), P(("dp", "sub"), None)),
        out_specs=(P("sub", None), P("dp", "sub"), P(None, "sub")),
        check_vma=False,
    )
```

```python
import functools

import jax
import jax.numpy as jnp
from jax import lax
from jax.experimental import pallas as pl
from jax.experimental.pallas import tpu as pltpu
from jax.sharding import PartitionSpec as P

M = 64
K = 256
LANES = 128
PIECES = 2


def contract_rows(left, right):
    return lax.dot_general(
        left, right, (((0,), (0,)), ((), ())), preferred_element_type=jnp.float32
    )


def plain_per_device(embeddings, rotation, centroids, assignments, codes):
    vec_rows, width = embeddings.shape
    cent_total = centroids.shape[0]
    sub_count = lax.axis_size("sub")
    dp_count = lax.axis_size("dp")
    total_rows = vec_rows * sub_count * dp_count
    gram_part = lax.psum_scatter(
        contract_rows(embeddings, embeddings).astype(jnp.bfloat16),
        "sub",
        scatter_dimension=0,
        tiled=True,
    ).astype(jnp.float32)
    rotated = jnp.dot(embeddings, rotation, preferred_element_type=jnp.float32)
    labels = lax.broadcasted_iota(jnp.int32, (1, cent_total), 1)
    select = (assignments[:, None] == labels).astype(jnp.bfloat16)
    base = jnp.dot(select, centroids, preferred_element_type=jnp.float32)
    residual = (rotated - base).astype(jnp.bfloat16)
    everything = contract_rows(select, residual)
    columns = lax.psum_scatter(
        everything.astype(jnp.bfloat16), "sub", scatter_dimension=1, tiled=True
    ).astype(jnp.float32)
    coarse = lax.psum_scatter(columns, "dp", scatter_dimension=0, tiled=True)
    coarse_sums = coarse * (cent_total / total_rows) ** 0.5
    code_words = codes.astype(jnp.bfloat16)
    moved, moved_codes = (
        lax.all_to_all(residual, "sub", split_axis=1, concat_axis=0, tiled=True),
        lax.all_to_all(code_words, "sub", split_axis=1, concat_axis=0, tiled=True),
    )
    local_m = codes.shape[1] // sub_count
    subw = width // codes.shape[1]
    owner_codes = moved_codes.astype(jnp.int32)
    gathered_rows = moved.shape[0]
    words = lax.broadcasted_iota(jnp.int32, (1, 1, K), 2)
    onehot = (owner_codes[:, :, None] == words).astype(jnp.bfloat16)
    pieces = moved.reshape(gathered_rows, local_m, subw)
    book_blocks = jnp.einsum("rmk,rms->kms", onehot, pieces, preferred_element_type=jnp.float32)
    book_local = book_blocks.reshape(K, local_m * subw)
    gram_sum, book_sum = lax.psum((gram_part, book_local), "dp")
    gram = gram_sum / total_rows
    codebook_sums = book_sum * (K / total_rows) ** 0.5
    return (gram, coarse_sums, codebook_sums)


def kernel(
    ns, nd, total_rows,
    emb, rot, cent, asg, codes,
    gram_o, coarse_o, book_o,
    gs1, gr1, gs2, gr2, gacc, gx, gs3, gr3, gy, gs4, gr4, gag,
    res, codes_t, ball, br1, bs2, br2, bacc, bs3, br3, bs4, br4, bag, cs3, cr3,
    ssem, rsem,
):
    rows, width = emb.shape
    cents = cent.shape[0]
    nh = ns // 2
    gr = width // ns
    pr = gr // PIECES
    cr = pr // nd
    bc = width // ns
    kr = K // nd
    f32, bf16 = jnp.float32, jnp.bfloat16
    d = lax.axis_index("dp")
    s = lax.axis_index("sub")
    half, par = s // 2, lax.rem(s, 2)
    nq = nd // 2
    dq, dpar = d // 2, lax.rem(d, 2)
    other = 1 - par
    pair = (d, half * 2 + other)

    def mate(k):
        return lax.rem(half + k, nh)

    def peer(k):
        return lax.rem(d + k, nd)

    barrier = pltpu.get_barrier_semaphore()
    greet = [pair]
    greet += [(d, mate(k) * 2 + par) for k in range(1, nh)]
    greet += [(peer(k), s) for k in range(1, nd)]
    for who in greet:
        pl.semaphore_signal(barrier, inc=1, device_id=who, device_id_type=pl.DeviceIdType.MESH)

    started = []

    def send(src, dst, who):
        n = len(started)
        copy = pltpu.make_async_remote_copy(
            src_ref=src, dst_ref=dst, send_sem=ssem.at[n], recv_sem=rsem.at[n],
            device_id=who, device_id_type=pl.DeviceIdType.MESH,
        )
        copy.start()
        started.append(copy)
        return copy

    def gram_block(q):
        cols = pl.ds(pl.multiple_of(q * gr, gr), gr)
        return contract_rows(emb[:, cols], emb[...]).astype(bf16)

    first = []
    for k in range(nh):
        i = mate(nh - 1 - k)
        gs1[k] = gram_block(i * 2 + other)
        if k == 0:
            pl.semaphore_wait(barrier, len(greet))
        first.append(send(gs1.at[k], gr1.at[k], pair))
    g2 = {}
    for k in range(nh):
        i = mate(nh - 1 - k)
        own = gram_block(i * 2 + par)
        first[k].wait_recv()
        both = own.astype(f32) + gr1[k].astype(f32)
        if k < nh - 1:
            gs2[k] = both.astype(bf16)
            who = (d, i * 2 + par)
            for h in range(PIECES):
                span = pl.ds(h * pr, pr)
                g2[k, h] = send(gs2.at[k, span], gr2.at[k, span], who)
        else:
            gacc[...] = both

    asg_row = asg[...]
    select = (asg_row == lax.broadcasted_iota(jnp.int32, (cents, rows), 0)).astype(f32).astype(bf16)
    for c in range(width // 256):
        cols = slice(c * 256, (c + 1) * 256)
        rotated = jnp.dot(emb[...], rot[:, cols], preferred_element_type=f32)
        base = contract_rows(select, cent[:, cols])
        res[:, cols] = (rotated - base).astype(bf16)
    m = codes.shape[1]
    eye = (
        lax.broadcasted_iota(jnp.int32, (m, m), 0) == lax.broadcasted_iota(jnp.int32, (m, m), 1)
    ).astype(f32).astype(bf16)
    codes_t[...] = lax.dot_general(
        eye, codes[...].astype(f32).astype(bf16), (((1,), (1,)), ((), ())),
        preferred_element_type=f32,
    ).astype(jnp.int32)

    subw = width // m
    per = LANES // subw
    lane_owner = lax.broadcasted_iota(jnp.int32, (K, LANES), 1) // subw
    words = lax.broadcasted_iota(jnp.int32, (K, rows), 0)
    groups = bc // LANES

    def group_step(g, carry):
        q, off = g // groups, lax.rem(g, groups)
        part = res[:, pl.ds(pl.multiple_of(g * LANES, LANES), LANES)]
        names = codes_t[pl.ds(pl.multiple_of(g * per, per), per), :]
        total = jnp.zeros((K, LANES), f32)
        for j in range(per):
            hot = jnp.where(names[j : j + 1, :] == words, 1.0, 0.0).astype(bf16)
            got = jnp.dot(hot, part, preferred_element_type=f32)
            total = jnp.where(lane_owner == j, got, total)
        lanes = pl.ds(pl.multiple_of(off * LANES, LANES), LANES)
        ball[q, 0:K, lanes] = total
        return carry

    lax.fori_loop(0, width // LANES, group_step, 0)
    cpad = ball.shape[1] - K
    select_pad = (asg_row == lax.broadcasted_iota(jnp.int32, (cpad, rows), 0)).astype(f32).astype(bf16)
    for q in range(ns):
        ball[q, K : K + cpad, :] = jnp.dot(
            select_pad, res[:, q * bc : (q + 1) * bc], preferred_element_type=f32
        )

    b1 = []
    for k in range(nh):
        i = mate(nh - 1 - k)
        b1.append(send(ball.at[i * 2 + other], br1.at[k], pair))
    b2 = {}
    for k in range(nh):
        i = mate(nh - 1 - k)
        b1[k].wait_recv()
        both = ball[i * 2 + par] + br1[k]
        if k < nh - 1:
            bs2[k] = both.astype(bf16)
            b2[k] = send(bs2.at[k], br2.at[k], (d, i * 2 + par))
        else:
            bacc[...] = both

    def quarter(k):
        return lax.rem(dq + k, nq)

    partner = (dq * 2 + 1 - dpar, s)
    g3 = {}
    for h in range(PIECES):
        span = pl.ds(h * pr, pr)
        total = gacc[span, :]
        for k in range(nh - 1):
            g2[k, h].wait_recv()
            total = total + gr2[k, span, :].astype(f32)
        split = total.reshape(nq, 2, cr, width)
        for e in range(2):
            gx[h, e] = split[:, e]
            gs3[h, e] = split[:, e].astype(bf16)
        g3[h] = send(gs3.at[h, 1 - dpar], gr3.at[h], partner)
    total = bacc[...]
    for k in range(nh - 1):
        b2[k].wait_recv()
        total = total + br2[k].astype(f32)
    split = total[0:K].reshape(nq, 2, kr, bc)
    for e in range(2):
        bs3[e] = split[:, e]
    b3 = send(bs3.at[1 - dpar], br3, partner)
    cper = cents // nd
    for e in range(nd):
        cs3[e] = total[K + e * cper : K + (e + 1) * cper]
    c3 = {}
    for k in range(1, nd):
        c3[k] = send(cs3.at[peer(k)], cr3.at[k - 1], (peer(k), s))

    g4 = {}
    for h in range(PIECES):
        g3[h].wait_recv()
        total = gx[h, dpar] + gr3[h].astype(f32)
        gy[h] = total
        gs4[h] = total.astype(bf16)
        for k in range(1, nq):
            g4[h, k] = send(gs4.at[h, quarter(k)], gr4.at[h, k - 1], (quarter(k) * 2 + dpar, s))
    b3.wait_recv()
    bs4[...] = bs3[dpar] + br3[...]
    b4 = {}
    for k in range(1, nq):
        b4[k] = send(bs4.at[quarter(k)], br4.at[k - 1], (quarter(k) * 2 + dpar, s))

    g5, b5 = {}, {}
    for h in range(PIECES):
        total = gy[h, dq]
        for k in range(1, nq):
            g4[h, k].wait_recv()
            total = total + gr4[h, k - 1].astype(f32)
        gag[h, d] = total.astype(bf16)
        for k in range(1, nq):
            g5[h, k] = send(gag.at[h, d], gag.at[h, d], (quarter(k) * 2 + dpar, s))
        g5[h, 0, "y"] = send(gag.at[h, d], gag.at[h, d], partner)
    total = bs4[dq]
    for k in range(1, nq):
        b4[k].wait_recv()
        total = total + br4[k - 1]
    bag[d] = total.astype(bf16)
    for k in range(1, nq):
        b5[k] = send(bag.at[d], bag.at[d], (quarter(k) * 2 + dpar, s))
    b5[0, "y"] = send(bag.at[d], bag.at[d], partner)
    for h in range(PIECES):
        for k in range(1, nq):
            g5[h, k].wait_recv()
            slot = quarter(nq - k) * 2 + dpar
            g5[h, k, "y"] = send(gag.at[h, slot], gag.at[h, slot], partner)
    for k in range(1, nq):
        b5[k].wait_recv()
        slot = quarter(nq - k) * 2 + dpar
        b5[k, "y"] = send(bag.at[slot], bag.at[slot], partner)
    ctotal = cs3[d]
    for k in range(1, nd):
        c3[k].wait_recv()
        ctotal = ctotal + cr3[k - 1]
    coarse_o[...] = ctotal * (cents / total_rows) ** 0.5
    for h in range(PIECES):
        for k in range(nq):
            g5[h, k, "y"].wait_recv()
        gram_o[h * pr : (h + 1) * pr, :] = gag[h].astype(f32).reshape(pr, width) * (1.0 / total_rows)
    for k in range(nq):
        b5[k, "y"].wait_recv()
    book_o[...] = bag[...].astype(f32).reshape(K, bc) * (K / total_rows) ** 0.5
    for copy in started:
        copy.wait_send()


def fused_per_device(ns, nd, embeddings, rotation, centroids, assignments, codes):
    rows, width = embeddings.shape
    cents = centroids.shape[0]
    total_rows = rows * ns * nd
    nh = ns // 2
    gr = width // ns
    pr = gr // PIECES
    cr = pr // nd
    bc = width // ns
    cpad = -(-cents // 16) * 16
    f32, bf16 = jnp.float32, jnp.bfloat16
    far = max(nh - 1, 1)
    nq = nd // 2
    kr = K // nd
    copies = nh + (nh - 1) * PIECES + nh + (nh - 1) + (PIECES + 1) * (3 * nq - 1) + nd - 1
    scratch = [
        pltpu.VMEM((nh, gr, width), bf16),
        pltpu.VMEM((nh, gr, width), bf16),
        pltpu.VMEM((far, gr, width), bf16),
        pltpu.VMEM((far, gr, width), bf16),
        pltpu.VMEM((gr, width), f32),
        pltpu.VMEM((PIECES, 2, nq, cr, width), f32),
        pltpu.VMEM((PIECES, 2, nq, cr, width), bf16),
        pltpu.VMEM((PIECES, nq, cr, width), bf16),
        pltpu.VMEM((PIECES, nq, cr, width), f32),
        pltpu.VMEM((PIECES, nq, cr, width), bf16),
        pltpu.VMEM((PIECES, nq - 1, cr, width), bf16),
        pltpu.VMEM((PIECES, nd, cr, width), bf16),
        pltpu.VMEM((rows, width), bf16),
        pltpu.VMEM((codes.shape[1], rows), jnp.int32),
        pltpu.VMEM((ns, K + cpad, bc), f32),
        pltpu.VMEM((nh, K + cpad, bc), f32),
        pltpu.VMEM((far, K + cpad, bc), bf16),
        pltpu.VMEM((far, K + cpad, bc), bf16),
        pltpu.VMEM((K + cpad, bc), f32),
        pltpu.VMEM((2, nq, kr, bc), f32),
        pltpu.VMEM((nq, kr, bc), f32),
        pltpu.VMEM((nq, kr, bc), f32),
        pltpu.VMEM((nq - 1, kr, bc), f32),
        pltpu.VMEM((nd, K // nd, bc), bf16),
        pltpu.VMEM((nd, cents // nd, bc), f32),
        pltpu.VMEM((nd - 1, cents // nd, bc), f32),
        pltpu.SemaphoreType.DMA((copies,)),
        pltpu.SemaphoreType.DMA((copies,)),
    ]
    vmem = pl.BlockSpec(memory_space=pltpu.VMEM)
    return tuple(
        pl.pallas_call(
            functools.partial(kernel, ns, nd, total_rows),
            out_shape=(
                jax.ShapeDtypeStruct((gr, width), f32),
                jax.ShapeDtypeStruct((cents // nd, bc), f32),
                jax.ShapeDtypeStruct((K, bc), f32),
            ),
            in_specs=[vmem] * 5,
            out_specs=(vmem,) * 3,
            scratch_shapes=scratch,
            compiler_params=pltpu.CompilerParams(
                collective_id=0, has_side_effects=True, vmem_limit_bytes=56 * 1024 * 1024
            ),
        )(embeddings, rotation, centroids, assignments.reshape(1, rows), codes)
    )


def solution(mesh):
    ns, nd = mesh.shape["sub"], mesh.shape["dp"]

    def per_device(embeddings, rotation, centroids, assignments, codes):
        rows, width = embeddings.shape
        cents = centroids.shape[0]
        fits = (
            ns % 2 == 0
            and nd > 2
            and nd % 2 == 0
            and width % (ns * PIECES * nd * 16) == 0
            and width % (ns * 2 * LANES // 2) == 0
            and K % (nd * 16) == 0
            and cents % nd == 0
            and cents % 8 == 0
            and LANES % (width // M) == 0
        )
        if fits:
            return fused_per_device(ns, nd, embeddings, rotation, centroids, assignments, codes)
        return plain_per_device(embeddings, rotation, centroids, assignments, codes)

    return jax.shard_map(
        per_device,
        mesh=mesh,
        in_specs=(P(("dp", "sub"), None), P(), P(), P(("dp", "sub")), P(("dp", "sub"), None)),
        out_specs=(P("sub", None), P("dp", "sub"), P(None, "sub")),
        check_vma=False,
    )
```

```python
import functools

import jax
import jax.numpy as jnp
from jax import lax
from jax.experimental import pallas as pl
from jax.experimental.pallas import tpu as pltpu
from jax.sharding import PartitionSpec as P

M = 64
K = 256
LANES = 128
PIECES = 2


def contract_rows(left, right):
    return lax.dot_general(
        left, right, (((0,), (0,)), ((), ())), preferred_element_type=jnp.float32
    )


def plain_per_device(embeddings, rotation, centroids, assignments, codes):
    vec_rows, width = embeddings.shape
    cent_total = centroids.shape[0]
    sub_count = lax.axis_size("sub")
    dp_count = lax.axis_size("dp")
    total_rows = vec_rows * sub_count * dp_count
    gram_part = lax.psum_scatter(
        contract_rows(embeddings, embeddings).astype(jnp.bfloat16),
        "sub",
        scatter_dimension=0,
        tiled=True,
    ).astype(jnp.float32)
    rotated = jnp.dot(embeddings, rotation, preferred_element_type=jnp.float32)
    labels = lax.broadcasted_iota(jnp.int32, (1, cent_total), 1)
    select = (assignments[:, None] == labels).astype(jnp.bfloat16)
    base = jnp.dot(select, centroids, preferred_element_type=jnp.float32)
    residual = (rotated - base).astype(jnp.bfloat16)
    everything = contract_rows(select, residual)
    columns = lax.psum_scatter(
        everything.astype(jnp.bfloat16), "sub", scatter_dimension=1, tiled=True
    ).astype(jnp.float32)
    coarse = lax.psum_scatter(columns, "dp", scatter_dimension=0, tiled=True)
    coarse_sums = coarse * (cent_total / total_rows) ** 0.5
    code_words = codes.astype(jnp.bfloat16)
    moved, moved_codes = (
        lax.all_to_all(residual, "sub", split_axis=1, concat_axis=0, tiled=True),
        lax.all_to_all(code_words, "sub", split_axis=1, concat_axis=0, tiled=True),
    )
    local_m = codes.shape[1] // sub_count
    subw = width // codes.shape[1]
    owner_codes = moved_codes.astype(jnp.int32)
    gathered_rows = moved.shape[0]
    words = lax.broadcasted_iota(jnp.int32, (1, 1, K), 2)
    onehot = (owner_codes[:, :, None] == words).astype(jnp.bfloat16)
    pieces = moved.reshape(gathered_rows, local_m, subw)
    book_blocks = jnp.einsum("rmk,rms->kms", onehot, pieces, preferred_element_type=jnp.float32)
    book_local = book_blocks.reshape(K, local_m * subw)
    gram_sum, book_sum = lax.psum((gram_part, book_local), "dp")
    gram = gram_sum / total_rows
    codebook_sums = book_sum * (K / total_rows) ** 0.5
    return (gram, coarse_sums, codebook_sums)


def kernel(
    ns, nd, total_rows,
    emb, rot, cent, asg, codes,
    gram_o, coarse_o, book_o,
    gs1, gr1, gs2, gr2, gacc, gx, gs3, gr3, gy, gs4, gr4, gag,
    res, codes_t, ball, br1, bs2, br2, bacc, bs3, br3, bs4, br4, bag, cs3, cr3,
    ssem, rsem,
):
    rows, width = emb.shape
    cents = cent.shape[0]
    nh = ns // 2
    gr = width // ns
    pr = gr // PIECES
    cr = pr // nd
    bc = width // ns
    kr = K // nd
    f32, bf16 = jnp.float32, jnp.bfloat16
    d = lax.axis_index("dp")
    s = lax.axis_index("sub")
    half, par = s // 2, lax.rem(s, 2)
    nq = nd // 2
    dq, dpar = d // 2, lax.rem(d, 2)
    other = 1 - par
    pair = (d, half * 2 + other)

    def mate(k):
        return lax.rem(half + k, nh)

    def peer(k):
        return lax.rem(d + k, nd)

    barrier = pltpu.get_barrier_semaphore()
    greet = [pair]
    greet += [(d, mate(k) * 2 + par) for k in range(1, nh)]
    greet += [(peer(k), s) for k in range(1, nd)]
    for who in greet:
        pl.semaphore_signal(barrier, inc=1, device_id=who, device_id_type=pl.DeviceIdType.MESH)

    started = []

    def send(src, dst, who):
        n = len(started)
        copy = pltpu.make_async_remote_copy(
            src_ref=src, dst_ref=dst, send_sem=ssem.at[n], recv_sem=rsem.at[n],
            device_id=who, device_id_type=pl.DeviceIdType.MESH,
        )
        copy.start()
        started.append(copy)
        return copy

    def gram_block(q):
        cols = pl.ds(pl.multiple_of(q * gr, gr), gr)
        return contract_rows(emb[:, cols], emb[...]).astype(bf16)

    first = []
    for k in range(nh):
        i = mate(nh - 1 - k)
        gs1[k] = gram_block(i * 2 + other)
        if k == 0:
            pl.semaphore_wait(barrier, len(greet))
        first.append(send(gs1.at[k], gr1.at[k], pair))
    g2 = {}
    for k in range(nh):
        i = mate(nh - 1 - k)
        own = gram_block(i * 2 + par)
        first[k].wait_recv()
        both = own.astype(f32) + gr1[k].astype(f32)
        if k < nh - 1:
            gs2[k] = both.astype(bf16)
            who = (d, i * 2 + par)
            for h in range(PIECES):
                span = pl.ds(h * pr, pr)
                g2[k, h] = send(gs2.at[k, span], gr2.at[k, span], who)
        else:
            gacc[...] = both

    asg_row = asg[...]
    select = (asg_row == lax.broadcasted_iota(jnp.int32, (cents, rows), 0)).astype(f32).astype(bf16)
    for c in range(width // 256):
        cols = slice(c * 256, (c + 1) * 256)
        rotated = jnp.dot(emb[...], rot[:, cols], preferred_element_type=f32)
        base = contract_rows(select, cent[:, cols])
        res[:, cols] = (rotated - base).astype(bf16)
    m = codes.shape[1]
    eye = (
        lax.broadcasted_iota(jnp.int32, (m, m), 0) == lax.broadcasted_iota(jnp.int32, (m, m), 1)
    ).astype(f32).astype(bf16)
    codes_t[...] = lax.dot_general(
        eye, codes[...].astype(f32).astype(bf16), (((1,), (1,)), ((), ())),
        preferred_element_type=f32,
    ).astype(jnp.int32)

    subw = width // m
    per = LANES // subw
    lane_owner = lax.broadcasted_iota(jnp.int32, (K, LANES), 1) // subw
    words = lax.broadcasted_iota(jnp.int32, (K, rows), 0)
    groups = bc // LANES

    def group_step(g, carry):
        q, off = g // groups, lax.rem(g, groups)
        part = res[:, pl.ds(pl.multiple_of(g * LANES, LANES), LANES)]
        names = codes_t[pl.ds(pl.multiple_of(g * per, per), per), :]
        total = jnp.zeros((K, LANES), f32)
        for j in range(per):
            hot = jnp.where(names[j : j + 1, :] == words, 1.0, 0.0).astype(bf16)
            got = jnp.dot(hot, part, preferred_element_type=f32)
            total = jnp.where(lane_owner == j, got, total)
        lanes = pl.ds(pl.multiple_of(off * LANES, LANES), LANES)
        ball[q, 0:K, lanes] = total
        return carry

    def quarter(k):
        return lax.rem(dq + k, nq)

    partner = (dq * 2 + 1 - dpar, s)
    g3 = {}
    def open_piece(h):
        span = pl.ds(h * pr, pr)
        total = gacc[span, :]
        for k in range(nh - 1):
            g2[k, h].wait_recv()
            total = total + gr2[k, span, :].astype(f32)
        split = total.reshape(nq, 2, cr, width)
        for e in range(2):
            gx[h, e] = split[:, e]
            gs3[h, e] = split[:, e].astype(bf16)
        g3[h] = send(gs3.at[h, 1 - dpar], gr3.at[h], partner)

    steps = width // LANES
    for h in range(PIECES):
        lax.fori_loop(steps * h // PIECES, steps * (h + 1) // PIECES, group_step, 0)
        open_piece(h)
    cpad = ball.shape[1] - K
    select_pad = (asg_row == lax.broadcasted_iota(jnp.int32, (cpad, rows), 0)).astype(f32).astype(bf16)
    for q in range(ns):
        ball[q, K : K + cpad, :] = jnp.dot(
            select_pad, res[:, q * bc : (q + 1) * bc], preferred_element_type=f32
        )

    b1 = []
    for k in range(nh):
        i = mate(nh - 1 - k)
        b1.append(send(ball.at[i * 2 + other], br1.at[k], pair))
    b2 = {}
    for k in range(nh):
        i = mate(nh - 1 - k)
        b1[k].wait_recv()
        both = ball[i * 2 + par] + br1[k]
        if k < nh - 1:
            bs2[k] = both.astype(bf16)
            b2[k] = send(bs2.at[k], br2.at[k], (d, i * 2 + par))
        else:
            bacc[...] = both

    total = bacc[...]
    for k in range(nh - 1):
        b2[k].wait_recv()
        total = total + br2[k].astype(f32)
    split = total[0:K].reshape(nq, 2, kr, bc)
    for e in range(2):
        bs3[e] = split[:, e]
    b3 = send(bs3.at[1 - dpar], br3, partner)
    cper = cents // nd
    for e in range(nd):
        cs3[e] = total[K + e * cper : K + (e + 1) * cper]
    c3 = {}
    for k in range(1, nd):
        c3[k] = send(cs3.at[peer(k)], cr3.at[k - 1], (peer(k), s))

    g4 = {}
    for h in range(PIECES):
        g3[h].wait_recv()
        total = gx[h, dpar] + gr3[h].astype(f32)
        gy[h] = total
        gs4[h] = total.astype(bf16)
        for k in range(1, nq):
            g4[h, k] = send(gs4.at[h, quarter(k)], gr4.at[h, k - 1], (quarter(k) * 2 + dpar, s))
    b3.wait_recv()
    bs4[...] = bs3[dpar] + br3[...]
    b4 = {}
    for k in range(1, nq):
        b4[k] = send(bs4.at[quarter(k)], br4.at[k - 1], (quarter(k) * 2 + dpar, s))

    g5, b5 = {}, {}
    for h in range(PIECES):
        total = gy[h, dq]
        for k in range(1, nq):
            g4[h, k].wait_recv()
            total = total + gr4[h, k - 1].astype(f32)
        gag[h, d] = total.astype(bf16)
        for k in range(1, nq):
            g5[h, k] = send(gag.at[h, d], gag.at[h, d], (quarter(k) * 2 + dpar, s))
        g5[h, 0, "y"] = send(gag.at[h, d], gag.at[h, d], partner)
    total = bs4[dq]
    for k in range(1, nq):
        b4[k].wait_recv()
        total = total + br4[k - 1]
    bag[d] = total.astype(bf16)
    for k in range(1, nq):
        b5[k] = send(bag.at[d], bag.at[d], (quarter(k) * 2 + dpar, s))
    b5[0, "y"] = send(bag.at[d], bag.at[d], partner)
    for h in range(PIECES):
        for k in range(1, nq):
            g5[h, k].wait_recv()
            slot = quarter(nq - k) * 2 + dpar
            g5[h, k, "y"] = send(gag.at[h, slot], gag.at[h, slot], partner)
    for k in range(1, nq):
        b5[k].wait_recv()
        slot = quarter(nq - k) * 2 + dpar
        b5[k, "y"] = send(bag.at[slot], bag.at[slot], partner)
    ctotal = cs3[d]
    for k in range(1, nd):
        c3[k].wait_recv()
        ctotal = ctotal + cr3[k - 1]
    coarse_o[...] = ctotal * (cents / total_rows) ** 0.5
    for h in range(PIECES):
        for k in range(nq):
            g5[h, k, "y"].wait_recv()
        gram_o[h * pr : (h + 1) * pr, :] = gag[h].astype(f32).reshape(pr, width) * (1.0 / total_rows)
    for k in range(nq):
        b5[k, "y"].wait_recv()
    book_o[...] = bag[...].astype(f32).reshape(K, bc) * (K / total_rows) ** 0.5
    for copy in started:
        copy.wait_send()


def fused_per_device(ns, nd, embeddings, rotation, centroids, assignments, codes):
    rows, width = embeddings.shape
    cents = centroids.shape[0]
    total_rows = rows * ns * nd
    nh = ns // 2
    gr = width // ns
    pr = gr // PIECES
    cr = pr // nd
    bc = width // ns
    cpad = -(-cents // 16) * 16
    f32, bf16 = jnp.float32, jnp.bfloat16
    far = max(nh - 1, 1)
    nq = nd // 2
    kr = K // nd
    copies = nh + (nh - 1) * PIECES + nh + (nh - 1) + (PIECES + 1) * (3 * nq - 1) + nd - 1
    scratch = [
        pltpu.VMEM((nh, gr, width), bf16),
        pltpu.VMEM((nh, gr, width), bf16),
        pltpu.VMEM((far, gr, width), bf16),
        pltpu.VMEM((far, gr, width), bf16),
        pltpu.VMEM((gr, width), f32),
        pltpu.VMEM((PIECES, 2, nq, cr, width), f32),
        pltpu.VMEM((PIECES, 2, nq, cr, width), bf16),
        pltpu.VMEM((PIECES, nq, cr, width), bf16),
        pltpu.VMEM((PIECES, nq, cr, width), f32),
        pltpu.VMEM((PIECES, nq, cr, width), bf16),
        pltpu.VMEM((PIECES, nq - 1, cr, width), bf16),
        pltpu.VMEM((PIECES, nd, cr, width), bf16),
        pltpu.VMEM((rows, width), bf16),
        pltpu.VMEM((codes.shape[1], rows), jnp.int32),
        pltpu.VMEM((ns, K + cpad, bc), f32),
        pltpu.VMEM((nh, K + cpad, bc), f32),
        pltpu.VMEM((far, K + cpad, bc), bf16),
        pltpu.VMEM((far, K + cpad, bc), bf16),
        pltpu.VMEM((K + cpad, bc), f32),
        pltpu.VMEM((2, nq, kr, bc), f32),
        pltpu.VMEM((nq, kr, bc), f32),
        pltpu.VMEM((nq, kr, bc), f32),
        pltpu.VMEM((nq - 1, kr, bc), f32),
        pltpu.VMEM((nd, K // nd, bc), bf16),
        pltpu.VMEM((nd, cents // nd, bc), f32),
        pltpu.VMEM((nd - 1, cents // nd, bc), f32),
        pltpu.SemaphoreType.DMA((copies,)),
        pltpu.SemaphoreType.DMA((copies,)),
    ]
    vmem = pl.BlockSpec(memory_space=pltpu.VMEM)
    return tuple(
        pl.pallas_call(
            functools.partial(kernel, ns, nd, total_rows),
            out_shape=(
                jax.ShapeDtypeStruct((gr, width), f32),
                jax.ShapeDtypeStruct((cents // nd, bc), f32),
                jax.ShapeDtypeStruct((K, bc), f32),
            ),
            in_specs=[vmem] * 5,
            out_specs=(vmem,) * 3,
            scratch_shapes=scratch,
            compiler_params=pltpu.CompilerParams(
                collective_id=0, has_side_effects=True, vmem_limit_bytes=56 * 1024 * 1024
            ),
        )(embeddings, rotation, centroids, assignments.reshape(1, rows), codes)
    )


def solution(mesh):
    ns, nd = mesh.shape["sub"], mesh.shape["dp"]

    def per_device(embeddings, rotation, centroids, assignments, codes):
        rows, width = embeddings.shape
        cents = centroids.shape[0]
        fits = (
            ns % 2 == 0
            and nd > 2
            and nd % 2 == 0
            and width % (ns * PIECES * nd * 16) == 0
            and width % (ns * 2 * LANES // 2) == 0
            and K % (nd * 16) == 0
            and cents % nd == 0
            and cents % 8 == 0
            and LANES % (width // M) == 0
        )
        if fits:
            return fused_per_device(ns, nd, embeddings, rotation, centroids, assignments, codes)
        return plain_per_device(embeddings, rotation, centroids, assignments, codes)

    return jax.shard_map(
        per_device,
        mesh=mesh,
        in_specs=(P(("dp", "sub"), None), P(), P(), P(("dp", "sub")), P(("dp", "sub"), None)),
        out_specs=(P("sub", None), P("dp", "sub"), P(None, "sub")),
        check_vma=False,
    )
```
